32 devices in a mesh: expert: 4 (over z), dp: 8 (over y, x, core).
Axes of the slice: x: 2, y: 2, z: 4, core: 2. Of those that a mesh axis runs over, the one named last changes fastest.
Arguments:
- tokens: bfloat16 [4096, 2048], P(('expert', 'dp')), may hold values from -6 to 6
- cotangent: bfloat16 [4096, 2048], P(('expert', 'dp')), may hold values from -1.796875 to 1.796875
- routes: int32 [4096, 8], P(('expert', 'dp')), may hold values from 0 to 127, as said below
- probs: float32 [4096, 8], P(('expert', 'dp')), may hold values from 0.05 to 0.5
- replicas: bfloat16 [4, 8, 2048, 1152], P('expert', 'dp'), as said below
- hold_now: int32 [4, 8], replicated, may hold values from 0 to 7, as said below
- hold_next: int32 [4, 8], replicated, may hold values from 0 to 7, as said below
- master: float32 [4, 2048, 2, 1152], P('expert', 'dp'), may hold values from -0.18 to 0.18
- moment: float32 [4, 2048, 2, 1152], P('expert', 'dp'), may hold values from -1.8 to 1.8
- second: float32 [4, 2048, 2, 1152], P('expert', 'dp'), may hold values from 0.01 to 1
Outputs:
- master_out: float32 [4, 2048, 2, 1152], P('expert', 'dp')
- moment_out: float32 [4, 2048, 2, 1152], P('expert', 'dp')
- second_out: float32 [4, 2048, 2, 1152], P('expert', 'dp')
- next_replicas: bfloat16 [4, 8, 2048, 1152], P('expert', 'dp')
The draws below stay inside these ranges and needn't reach their ends.
Inputs may be any that keep to these rules, and one draw needn't show every extreme that they name: `routes`: each token names 8 different experts of the layer; in every block of 128 tokens some expert of the window is named by at least 24 tokens. `hold_now`: slice 2 e + h is half h of window expert e; every slice is held by at least 2 devices, and some slice by exactly 2. `hold_next`: slice 2 e + h is half h of window expert e. replicas[a, j] holds slice hold_now[a, j]; devices that hold the same slice hold equal values.
All inputs are finite; a program needn't handle non-finite values.
Results may differ from the reference program's by a relative error of at most 0.001.
Values may be sent and summed in bfloat16 or wider, within the bound.
No kernel may reach another device: no remote copies, remote signals or barrier semaphores. Data moves between devices by JAX's collectives and lax.ppermute only.
A program may use at most 128 MiB of HBM per device.

```python
import math
import jax
import jax.numpy as jnp
from jax import lax

D = 2048
NE_ALL = 128
TOP = 8
TOK_DEV = 128
EXPERTS = 4
TOKENS = 4096
HALFW = 1152
CAP = 24
N_EXPERT = 4
N_DP = 8


def hot_expert(key):
    return jax.random.randint(jax.random.fold_in(key, 5), (), 0, EXPERTS)


def holder_map(key, hot):
    pieces = 2 * EXPERTS
    devices = N_EXPERT * N_DP
    fewest = N_DP // 4
    spare = devices - pieces * fewest
    hot_piece = 2 * hot
    extra = jax.random.randint(jax.random.fold_in(key, 6), (spare,), 0, pieces - 1)
    extra = extra + (extra >= hot_piece).astype(jnp.int32)
    base_list = jnp.repeat(jnp.arange(pieces, dtype=jnp.int32), fewest)
    listing = jnp.concatenate([base_list, extra.astype(jnp.int32)])
    shuffle = jax.random.permutation(jax.random.fold_in(key, 7), devices)
    return listing[shuffle].reshape(N_EXPERT, N_DP).astype(jnp.int32)


def draw_hold_now(key, part):
    return holder_map(jax.random.fold_in(key, 11), hot_expert(key))


def draw_hold_next(key, part):
    own_key = jax.random.fold_in(key, 12)
    return holder_map(own_key, hot_expert(own_key))


def draw_replicas(key, part):
    holdings = draw_hold_now(key, part).reshape(-1)
    base_key = jax.random.fold_in(key, 21)
    base_values = 0.03 * jax.random.normal(base_key, (2 * EXPERTS, D, HALFW), jnp.float32)
    base_values = base_values.astype(jnp.bfloat16)
    return base_values[holdings].reshape(N_EXPERT, N_DP, D, HALFW)


def draw_routes(key, part):
    hot = hot_expert(key)
    tokens_all = TOK_DEV * N_EXPERT * N_DP
    block_total = N_EXPERT * N_DP
    bias = jax.random.randint(jax.random.fold_in(key, 31), (NE_ALL,), 0, 4)
    noise = jax.random.randint(jax.random.fold_in(key, 32), (tokens_all, NE_ALL), 0, 1 << 16)
    scores = (noise + bias[None, :] * (1 << 14)) * NE_ALL + jnp.arange(NE_ALL, dtype=jnp.int32)[None, :]
    picked = lax.top_k(scores, TOP)[1].astype(jnp.int32)
    draws = jax.random.randint(jax.random.fold_in(key, 33), (block_total, TOK_DEV), 0, 1 << 20)
    keyed = draws * TOK_DEV + jnp.arange(TOK_DEV, dtype=jnp.int32)[None, :]
    ranked = jnp.argsort(jnp.argsort(keyed, axis=1), axis=1)
    forced = (ranked < CAP + CAP // 2).reshape(-1)
    present = jnp.any(picked == hot, axis=1)
    last_pick = jnp.where(forced & jnp.logical_not(present), hot, picked[:, TOP - 1])
    return jnp.concatenate([picked[:, :TOP - 1], last_pick[:, None]], axis=1).astype(jnp.int32)


def block_scale(stream_key, dims, split, smallest, top_value):
    factor_of, own = 1.0, jax.random.fold_in(stream_key, 6)
    for dim, blocks in split:
        steps = jnp.exp(jax.random.uniform(jax.random.fold_in(own, dim), (blocks,), jnp.float32, smallest / len(split), top_value / len(split)))
        factor_of = factor_of * jnp.repeat(steps, dims[dim] // blocks).reshape([-1 if axis == dim else 1 for axis in range(len(dims))])
    return factor_of


def centred(key, shape, spread, limit, shards=(), held_as=jnp.bfloat16):
    array = jax.random.normal(key, shape, jnp.float32) * spread
    if len(shards) > 0:
        array = block_scale(key, shape, shards, -0.22, 0.18) * array
    return jnp.clip(array, min=-limit, max=limit).astype(held_as)


def setup_inputs(seed: int = 0) -> dict:
    seeds = jax.random.split(jax.random.key(seed), 11)
    tokens = centred(seeds[0], (TOKENS, D), 1.0, 6.0, ((0, 32),))
    cotangent = centred(seeds[1], (TOKENS, D), 0.3, 1.796875, ((0, 32),))
    routes = draw_routes(jax.random.fold_in(seeds[10], 71), 0)
    probs = jnp.clip(0.05 + 0.45 * jax.random.uniform(seeds[3], (TOKENS, TOP), jnp.float32) ** block_scale(seeds[3], (TOKENS, TOP), ((0, 32),), -0.2, 0.2), 0.05, 0.5)
    replicas = draw_replicas(jax.random.fold_in(seeds[10], 71), 0)
    hold_now = draw_hold_now(jax.random.fold_in(seeds[10], 71), 0)
    hold_next = draw_hold_next(jax.random.fold_in(seeds[10], 71), 0)
    master = centred(seeds[7], (EXPERTS, D, 2, HALFW), 0.03, 0.18, ((0, 4), (1, 8)), jnp.float32)
    moment = centred(seeds[8], (EXPERTS, D, 2, HALFW), 0.3, 1.8, ((0, 4), (1, 8)), jnp.float32)
    second = jnp.clip(jnp.exp(math.log(1.0) - 4.6051702 * jax.random.uniform(seeds[9], (EXPERTS, D, 2, HALFW), jnp.float32) ** block_scale(seeds[9], (EXPERTS, D, 2, HALFW), ((0, 4), (1, 8)), -0.2, 0.2)), 0.01, 1.0)
    return dict(tokens=tokens, cotangent=cotangent, routes=routes, probs=probs, replicas=replicas, hold_now=hold_now, hold_next=hold_next, master=master, moment=moment, second=second)


beta_one = 0.9
beta_two = 0.999
learn_rate = 0.01
decay_rate = 0.1
adam_eps = 1e-08
adam_count = 20.0

def half_grads(rows_in, rows_out, weight):
    half_width = weight.shape[1] // 3
    preact = jnp.dot(rows_in, weight[:, :2 * half_width], preferred_element_type=jnp.float32)
    gate_pre = preact[:, :half_width]
    up_pre = preact[:, half_width:]
    sig_gate = jax.nn.sigmoid(gate_pre)
    activated = gate_pre * sig_gate
    hidden = (activated * up_pre).astype(jnp.bfloat16)
    hidden_grad = jnp.dot(rows_out, weight[:, 2 * half_width:], preferred_element_type=jnp.float32)
    gate_grad = hidden_grad * up_pre * sig_gate * (1.0 + gate_pre * (1.0 - sig_gate))
    pre_grad = jnp.concatenate([gate_grad, hidden_grad * activated], axis=1).astype(jnp.bfloat16)
    grad_in = lax.dot_general(rows_in, pre_grad, (((0,), (0,)), ((), ())), preferred_element_type=jnp.float32)
    grad_out = lax.dot_general(rows_out, hidden, (((0,), (0,)), ((), ())), preferred_element_type=jnp.float32)
    return jnp.concatenate([grad_in, grad_out], axis=1)

def adam_step(master, moment, second, gradient):
    moment_out = beta_one * moment + (1.0 - beta_one) * gradient
    second_out = beta_two * second + (1.0 - beta_two) * gradient * gradient
    scale_one = 1.0 - beta_one ** adam_count
    scale_two = 1.0 - beta_two ** adam_count
    update = moment_out / scale_one / (jnp.sqrt(second_out / scale_two) + adam_eps)
    master_out = master - learn_rate * (update + decay_rate * master)
    return (master_out, moment_out, second_out)

def reference(tokens, cotangent, routes, probs, replicas, hold_now, hold_next, master, moment, second):
    block_total = tokens.shape[0] // TOK_DEV
    devices = N_EXPERT * N_DP
    flat_hold = hold_now.reshape(devices)
    flat_replicas = replicas.reshape(devices, D, HALFW)
    device_ids = jnp.arange(devices, dtype=jnp.int32)
    slot_ids = jnp.arange(CAP, dtype=jnp.int32)
    places = jnp.arange(TOK_DEV, dtype=jnp.int32)
    block_ids = jnp.arange(block_total, dtype=jnp.int32)

    def one_expert(expert):
        picked = routes == expert
        member = jnp.any(picked, axis=1).astype(jnp.int32).reshape(block_total, TOK_DEV)
        weight_row = lax.optimization_barrier(jnp.sum(jnp.where(picked, probs, 0.0), axis=1))
        ranked = jnp.cumsum(member, axis=1) - member
        hit_table = (member[:, :, None] == 1) & (ranked[:, :, None] == slot_ids[None, None, :])
        place_in = lax.optimization_barrier(jnp.sum(jnp.where(hit_table, places[None, :, None], 0), axis=1)).astype(jnp.int32)
        filled = jnp.any(hit_table, axis=1).reshape(-1)
        token_ids = (place_in + block_ids[:, None] * TOK_DEV).reshape(-1).astype(jnp.int32)
        rows_in = jnp.where(filled[:, None], tokens[token_ids], 0).astype(tokens.dtype)
        scaled = (weight_row[token_ids][:, None] * cotangent[token_ids]).astype(jnp.bfloat16)
        rows_out = jnp.where(filled[:, None], scaled, 0).astype(jnp.bfloat16)
        halves = []
        for half_index in range(2):
            slice_id = 2 * expert + half_index
            first_holder = jnp.min(jnp.where(flat_hold == slice_id, device_ids, devices)).astype(jnp.int32)
            weight = flat_replicas[first_holder]
            halves.append(half_grads(rows_in, rows_out, weight))
        return jnp.stack(halves, axis=1)
    gradient = lax.map(one_expert, jnp.arange(EXPERTS, dtype=jnp.int32))
    master_out, moment_out, second_out = adam_step(master, moment, second, gradient)
    fresh = master_out.astype(jnp.bfloat16)
    flat_next = hold_next.reshape(devices)
    chosen = fresh[flat_next // 2, :, flat_next % 2, :]
    next_replicas = chosen.reshape(N_EXPERT, N_DP, D, HALFW)
    return (master_out, moment_out, second_out, next_replicas)
```

```python
import functools

import jax
import jax.numpy as jnp
from jax import lax
from jax.experimental import pallas as pl
from jax.experimental.pallas import tpu as pltpu
from jax.sharding import PartitionSpec as P

CAP = 24

beta_one = 0.9
beta_two = 0.999
learn_rate = 0.01
decay_rate = 0.1
adam_eps = 1e-08
adam_count = 20.0

VMEM_LIMIT = 60 * 1024 * 1024


def adam_step(master, moment, second, gradient):
    moment_out = beta_one * moment + (1.0 - beta_one) * gradient
    second_out = beta_two * second + (1.0 - beta_two) * gradient * gradient
    scale_one = 1.0 - beta_one**adam_count
    scale_two = 1.0 - beta_two**adam_count
    update = moment_out / scale_one / (jnp.sqrt(second_out / scale_two) + adam_eps)
    master_out = master - learn_rate * (update + decay_rate * master)
    return (master_out, moment_out, second_out)


def keep_kernel(count, place_ref, routes_ref, probs_ref, tokens_ref, cot_ref, *out_refs):
    token_count = tokens_ref.shape[0]
    routes = routes_ref[...]
    probs = probs_ref[...]
    members = []
    factors = []
    for step in range(count):
        expert = lax.rem(place_ref[0] + step, count)
        picked = routes == expert
        members.append(jnp.sum(jnp.where(picked, 1.0, 0.0), axis=0, keepdims=True))
        factors.append(jnp.sum(jnp.where(picked, probs, 0.0), axis=0, keepdims=True))
    table = jnp.concatenate(members + [jnp.zeros_like(members[0])] * (-count % 8), axis=0)
    earlier = lax.broadcasted_iota(jnp.int32, (token_count, token_count), 0)
    later = lax.broadcasted_iota(jnp.int32, (token_count, token_count), 1)
    before = jnp.where(earlier < later, 1.0, 0.0).astype(jnp.bfloat16)
    ranked = jnp.dot(table.astype(jnp.bfloat16), before, preferred_element_type=jnp.float32)
    slots = lax.broadcasted_iota(jnp.int32, (CAP, token_count), 0).astype(jnp.float32)
    hits = []
    scales = []
    for step in range(count):
        hit = (members[step] > 0.5) & (ranked[step : step + 1] == slots)
        hits.append(jnp.where(hit, 1.0, 0.0))
        scales.append(jnp.sum(jnp.where(hit, factors[step], 0.0), axis=1, keepdims=True))
    one_hot = jnp.concatenate(hits, axis=0).astype(jnp.bfloat16)
    scale = jnp.concatenate(scales, axis=0)
    rows_in = jnp.dot(one_hot, tokens_ref[...], preferred_element_type=jnp.float32)
    rows_out = scale * jnp.dot(one_hot, cot_ref[...], preferred_element_type=jnp.float32)
    for step in range(count):
        span = slice(step * CAP, (step + 1) * CAP)
        out_refs[step][0] = rows_in[span].astype(jnp.bfloat16)
        out_refs[step][1] = rows_out[span].astype(jnp.bfloat16)


def keep_rows(tokens, cotangent, routes, probs, place, count):
    width = tokens.shape[1]
    vmem = pl.BlockSpec(memory_space=pltpu.VMEM)
    return pl.pallas_call(
        functools.partial(keep_kernel, count),
        out_shape=[jax.ShapeDtypeStruct((2, CAP, width), jnp.bfloat16)] * count,
        in_specs=[pl.BlockSpec(memory_space=pltpu.SMEM)] + [vmem] * 4,
        out_specs=[vmem] * count,
        cost_estimate=pl.CostEstimate(flops=4_000_000_000, bytes_accessed=2_000_000, transcendentals=0),
        name="keep_rows",
    )(place, routes.T, probs.T, tokens, cotangent)


def turn_kernel(parts, part_ref, weight_ref, out_ref):
    turned = weight_ref[...].astype(jnp.float32).T
    half_width = turned.shape[0] // 3
    units = half_width // parts
    for piece in range(parts):
        rows = [
            turned[kind * half_width + piece * units : kind * half_width + (piece + 1) * units]
            for kind in range(3)
        ]
        out_ref[piece] = jnp.concatenate(rows, axis=0).astype(jnp.bfloat16)


def turn_weights(weight, part, parts):
    width, columns = weight.shape
    span = width // 2
    block = min(256, span)
    steps = span // block
    return pl.pallas_call(
        functools.partial(turn_kernel, parts),
        out_shape=jax.ShapeDtypeStruct((parts, columns // parts, span), jnp.bfloat16),
        grid_spec=pltpu.PrefetchScalarGridSpec(
            num_scalar_prefetch=1,
            grid=(steps,),
            in_specs=[pl.BlockSpec((block, columns), lambda i, part: (part[0] * steps + i, 0))],
            out_specs=pl.BlockSpec((parts, columns // parts, block), lambda i, part: (0, 0, i)),
        ),
        cost_estimate=pl.CostEstimate(flops=4_000_000_000, bytes_accessed=5_000_000, transcendentals=0),
        name="turn_weights",
    )(part, weight)


def pick_kernel(table_ref, own_ref, old_ref, out_ref):
    unit = pl.program_id(0)

    @pl.when(table_ref[0, unit] == 1)
    def _():
        out_ref[...] = own_ref[...]

    @pl.when(table_ref[0, unit] == 0)
    def _():
        out_ref[...] = old_ref[...]


def pick_units(table, pieces, old):
    count, rows, span = old.shape
    return pl.pallas_call(
        pick_kernel,
        out_shape=jax.ShapeDtypeStruct(old.shape, old.dtype),
        grid_spec=pltpu.PrefetchScalarGridSpec(
            num_scalar_prefetch=1,
            grid=(count,),
            in_specs=[
                pl.BlockSpec((1, rows, span), lambda i, table: (table[1, i], 0, 0)),
                pl.BlockSpec((1, rows, span), lambda i, table: (i, 0, 0)),
            ],
            out_specs=pl.BlockSpec((1, rows, span), lambda i, table: (i, 0, 0)),
        ),
        cost_estimate=pl.CostEstimate(flops=1_000_000_000, bytes_accessed=4_000_000, transcendentals=0),
        name="pick_units",
    )(table, pieces, old)


def grad_kernel(count, chunks, table_ref, own_ref, left_ref, right_ref, *refs):
    ins = refs[:count]
    outs = refs[count : 2 * count]
    grads = refs[2 * count : 2 * count + chunks]
    rows_in, rows_out, pair_w, down_w, pair_g, down_g, sems = refs[2 * count + chunks :]
    rows = ins[0].shape[0]
    units = down_w.shape[0] // 2
    span = own_ref.shape[2]
    width = rows_in.shape[1]

    copies = []
    for index in range(count):
        place = pl.ds(index * rows, rows)
        copies.append(pltpu.make_async_copy(ins[index], rows_in.at[place], sems.at[0, index]))
        copies.append(pltpu.make_async_copy(outs[index], rows_out.at[place], sems.at[1, index]))
    for copy in copies:
        copy.start()

    for unit in range(4):
        half, part = unit // 2, unit % 2
        lanes = pl.ds(part * span, span)

        def fetch(source, unit=unit, half=half, lanes=lanes):
            one = pltpu.make_async_copy(
                source.at[pl.ds(0, 2 * units)],
                pair_w.at[pl.ds(2 * half * units, 2 * units), lanes],
                sems.at[2, 2 * unit],
            )
            two = pltpu.make_async_copy(
                source.at[pl.ds(2 * units, units)],
                down_w.at[pl.ds(half * units, units), lanes],
                sems.at[2, 2 * unit + 1],
            )
            one.start()
            two.start()
            one.wait()
            two.wait()

        @pl.when(table_ref[0, unit] == 0)
        def _(unit=unit, fetch=fetch):
            fetch(own_ref.at[table_ref[1, unit]])

        @pl.when(table_ref[0, unit] == 1)
        def _(unit=unit, fetch=fetch):
            fetch(left_ref.at[unit])

        @pl.when(table_ref[0, unit] == 2)
        def _(unit=unit, fetch=fetch):
            fetch(right_ref.at[unit])

    for copy in copies:
        copy.wait()

    contract = (((1,), (1,)), ((), ()))
    pair = lax.dot_general(pair_w[...], rows_in[...], contract, preferred_element_type=jnp.float32)
    down = lax.dot_general(down_w[...], rows_out[...], contract, preferred_element_type=jnp.float32)
    for half in range(2):
        gate = pair[2 * half * units : (2 * half + 1) * units]
        up = pair[(2 * half + 1) * units : (2 * half + 2) * units]
        hidden_grad = down[half * units : (half + 1) * units]
        sig = jax.nn.sigmoid(gate)
        activated = gate * sig
        down_g[pl.ds(half * units, units)] = (activated * up).astype(jnp.bfloat16)
        gate_grad = hidden_grad * up * sig * (1.0 + gate * (1.0 - sig))
        pair_g[pl.ds(2 * half * units, 2 * units)] = jnp.concatenate(
            [gate_grad, hidden_grad * activated], axis=0
        ).astype(jnp.bfloat16)

    owners = grads[0].shape[0]
    block = width // owners
    lane = block // chunks

    def owner_step(owner, carry):
        place = pl.ds(pl.multiple_of(owner * block, block), block)
        grad_in = jnp.dot(pair_g[...], rows_in[:, place], preferred_element_type=jnp.float32)
        grad_out = jnp.dot(down_g[...], rows_out[:, place], preferred_element_type=jnp.float32)
        for chunk in range(chunks):
            part = slice(chunk * lane, (chunk + 1) * lane)
            for half in range(2):
                grads[chunk][owner, pl.ds(3 * half * units, 2 * units)] = grad_in[
                    2 * half * units : (2 * half + 2) * units, part
                ]
                grads[chunk][owner, pl.ds((3 * half + 2) * units, units)] = grad_out[
                    half * units : (half + 1) * units, part
                ]
        return carry

    lax.fori_loop(0, owners, owner_step, 0)


def half_grads(table, own, left, right, ins, outs, owners, chunks):
    count = len(ins)
    rows, width = ins[0].shape
    units = own.shape[1] // 3
    tokens = count * rows
    anywhere = pl.BlockSpec(memory_space=pl.ANY)
    lane = width // owners // chunks
    return pl.pallas_call(
        functools.partial(grad_kernel, count, chunks),
        out_shape=[jax.ShapeDtypeStruct((owners, 6 * units, lane), jnp.float32)] * chunks,
        in_specs=[pl.BlockSpec(memory_space=pltpu.SMEM)] + [anywhere] * (3 + 2 * count),
        out_specs=[pl.BlockSpec(memory_space=pltpu.VMEM)] * chunks,
        scratch_shapes=[
            pltpu.VMEM((tokens, width), jnp.bfloat16),
            pltpu.VMEM((tokens, width), jnp.bfloat16),
            pltpu.VMEM((4 * units, width), jnp.bfloat16),
            pltpu.VMEM((2 * units, width), jnp.bfloat16),
            pltpu.VMEM((4 * units, tokens), jnp.bfloat16),
            pltpu.VMEM((2 * units, tokens), jnp.bfloat16),
            pltpu.SemaphoreType.DMA((3, max(8, count))),
        ],
        compiler_params=pltpu.CompilerParams(vmem_limit_bytes=VMEM_LIMIT),
        cost_estimate=pl.CostEstimate(flops=10_000_000_000, bytes_accessed=10_000_000, transcendentals=0),
        name="half_grads",
    )(table, own, left, right, *ins, *outs)


def rows_kernel(arrived_ref, out_ref):
    parts, lines, _ = arrived_ref.shape
    units = lines // 6
    for half in range(2):
        stacked = jnp.concatenate(
            [
                arrived_ref[part, pl.ds((3 * half + kind) * units, units)]
                for kind in range(3)
                for part in range(parts)
            ],
            axis=0,
        )
        out_ref[half] = stacked.T


def gradient_rows(arrived):
    parts, lines, lane = arrived.shape
    return pl.pallas_call(
        rows_kernel,
        out_shape=jax.ShapeDtypeStruct((2, lane, parts * lines // 2), jnp.float32),
        in_specs=[pl.BlockSpec(memory_space=pltpu.VMEM)],
        out_specs=pl.BlockSpec(memory_space=pltpu.VMEM),
        compiler_params=pltpu.CompilerParams(vmem_limit_bytes=VMEM_LIMIT),
        cost_estimate=pl.CostEstimate(flops=2_000_000_000, bytes_accessed=5_000_000, transcendentals=0),
        name="gradient_rows",
    )(arrived)


def choose_kernel(count, want_ref, *refs):
    sources = refs[:count]
    out_ref = refs[count]
    for slot in range(out_ref.shape[0]):
        for index in range(count):

            @pl.when(want_ref[slot] == index)
            def _(slot=slot, index=index):
                out_ref[slot] = sources[index][...]


def choose_pieces(want, sources):
    count = len(sources)
    slots = want.shape[0]
    rows, columns = sources[0].shape
    vmem = pl.BlockSpec(memory_space=pltpu.VMEM)
    return pl.pallas_call(
        functools.partial(choose_kernel, count),
        out_shape=jax.ShapeDtypeStruct((slots, rows, columns), sources[0].dtype),
        in_specs=[pl.BlockSpec(memory_space=pltpu.SMEM)] + [vmem] * count,
        out_specs=vmem,
        compiler_params=pltpu.CompilerParams(vmem_limit_bytes=VMEM_LIMIT),
        cost_estimate=pl.CostEstimate(flops=1_500_000_000, bytes_accessed=4_000_000, transcendentals=0),
        name="choose_pieces",
    )(want, *sources)


def swap(value, mask, count):
    return lax.ppermute(value, "dp", [(i, i ^ mask) for i in range(count)])


def gather_rows(pieces, count):
    masks = [1 << bit for bit in range(count.bit_length() - 1)]
    while len(masks) >= 2:
        two, one = masks.pop(), masks.pop()
        grown = []
        for piece in pieces:
            first = [swap(half, one, count) for half in piece]
            other = [swap(half, two, count) for half in piece]
            far = (swap(first[0], two, count), swap(other[1], one, count))
            grown += [piece, tuple(first), tuple(other), far]
        pieces = grown
    if masks:
        pieces = pieces + [tuple(swap(half, masks[0], count) for half in piece) for piece in pieces]
    return pieces


def body(tokens, cotangent, routes, probs, replicas, hold_now, hold_next, master, moment, second):
    planes = lax.axis_size("expert")
    columns = lax.axis_size("dp")
    devices = planes * columns
    width = tokens.shape[1]
    block_rows = width // columns
    plane = lax.axis_index("expert")
    column = lax.axis_index("dp")

    kept = keep_rows(tokens, cotangent, routes, probs, plane.reshape(1), planes)
    came = [kept[0]] + [
        lax.ppermute(kept[step], "expert", [(i, (i + step) % planes) for i in range(planes)])
        for step in range(1, planes)
    ]

    flat = hold_now.reshape(devices)
    ids = jnp.arange(devices, dtype=jnp.int32)
    order = jnp.abs(ids // columns - flat // 2) * devices + ids
    ahead = (flat[:, None] == flat[None, :]) & (order[None, :] < order[:, None])
    rank = jnp.sum(ahead.astype(jnp.int32), axis=1)
    pieces_ids = jnp.arange(2 * planes, dtype=jnp.int32)
    chosen = (flat[None, None, :] == pieces_ids[:, None, None]) & (
        rank[None, None, :] == jnp.arange(2, dtype=jnp.int32)[None, :, None]
    )
    holder = jnp.sum(jnp.where(chosen, ids[None, None, :], 0), axis=2)
    from_plane = (holder // columns).reshape(planes, 4)
    from_column = (holder % columns).reshape(planes, 4)
    hops = jnp.max(jnp.abs(from_plane - jnp.arange(planes, dtype=jnp.int32)[:, None]))
    my_rank = jnp.sum(jnp.where(ids == plane * columns + column, rank, 0))
    my_part = (my_rank == 1).astype(jnp.int32).reshape(1)

    turned = turn_weights(replicas[0, 0], my_part, columns)
    own = lax.all_to_all(turned, "dp", split_axis=0, concat_axis=0, tiled=True)

    def plan(target):
        at = jnp.clip(target, 0, planes - 1)
        planes_of = lax.dynamic_index_in_dim(from_plane, at, 0, keepdims=False)
        columns_of = lax.dynamic_index_in_dim(from_column, at, 0, keepdims=False)
        return planes_of, columns_of

    def hop(index, carry):
        left, right = carry
        step = hops - index
        up_planes, up_columns = plan(plane + step)
        down_planes, down_columns = plan(plane - step)
        up_table = jnp.stack([(up_planes == plane).astype(jnp.int32), up_columns])
        down_table = jnp.stack([(down_planes == plane).astype(jnp.int32), down_columns])
        up = pick_units(up_table, own, left)
        down = pick_units(down_table, own, right)
        left = lax.ppermute(up, "expert", [(i, i + 1) for i in range(planes - 1)])
        right = lax.ppermute(down, "expert", [(i + 1, i) for i in range(planes - 1)])
        return left, right

    empty = jnp.zeros((4,) + own.shape[1:], own.dtype)
    left, right = lax.fori_loop(0, hops, hop, (empty, empty))
    my_planes, my_columns = plan(plane)
    side = jnp.where(my_planes == plane, 0, jnp.where(my_planes < plane, 1, 2)).astype(jnp.int32)
    table = jnp.stack([side, my_columns])

    first = (
        jnp.concatenate([rows[0] for rows in came], axis=0),
        jnp.concatenate([rows[1] for rows in came], axis=0),
    )
    rows = gather_rows([first], columns)

    chunks = max(1, block_rows // 128)
    partial = half_grads(
        table, own, left, right, [r[0] for r in rows], [r[1] for r in rows], columns, chunks
    )
    lane = block_rows // chunks
    gradients = [
        gradient_rows(lax.all_to_all(part, "dp", split_axis=0, concat_axis=0, tiled=True))
        for part in partial
    ]

    next_row = lax.dynamic_index_in_dim(hold_next, plane, 0, keepdims=False)
    next_plane = next_row // 2
    next_half = next_row % 2
    turns = jnp.where(next_half == 0, plane - next_plane, next_plane - plane)
    want = (next_half * planes + (turns + planes) % planes).astype(jnp.int32)
    forward = [(i, (i + 1) % planes) for i in range(planes)]
    backward = [(i, (i - 1) % planes) for i in range(planes)]
    arrived = []
    splits = 2 if lane % 32 == 0 else 1
    for chunk in range(chunks):
        for split in range(splits):
            size = lane // splits
            begin = chunk * lane + split * size
            span = slice(begin, begin + size)
            grad = jnp.transpose(gradients[chunk][:, split * size : (split + 1) * size], (1, 0, 2))
            fresh = adam_step(master[0, span], moment[0, span], second[0, span], grad)[0]
            fresh = fresh.astype(jnp.bfloat16)
            rings = [[fresh[:, 0]], [fresh[:, 1]]]
            for _ in range(planes - 1):
                rings[0].append(lax.ppermute(rings[0][-1], "expert", forward))
                rings[1].append(lax.ppermute(rings[1][-1], "expert", backward))
            outgoing = choose_pieces(want, rings[0] + rings[1])
            arrived.append(lax.all_to_all(outgoing, "dp", split_axis=0, concat_axis=0, tiled=True))
    next_replicas = jnp.concatenate(arrived, axis=1).reshape(1, 1, width, arrived[0].shape[2])

    gradient = jnp.transpose(jnp.concatenate(gradients, axis=1), (1, 0, 2))[None]
    master_out, moment_out, second_out = adam_step(master, moment, second, gradient)
    return (master_out, moment_out, second_out, next_replicas)


def solution(mesh):
    placed = (
        P(("expert", "dp"), None),
        P(("expert", "dp"), None),
        P(("expert", "dp"), None),
        P(("expert", "dp"), None),
        P("expert", "dp", None, None),
        P(),
        P(),
        P("expert", "dp", None, None),
        P("expert", "dp", None, None),
        P("expert", "dp", None, None),
    )
    return jax.shard_map(
        body,
        mesh=mesh,
        in_specs=placed,
        out_specs=(P("expert", "dp", None, None),) * 4,
        check_vma=False,
    )
```

```python
import functools

import jax
import jax.numpy as jnp
from jax import lax
from jax.experimental import pallas as pl
from jax.experimental.pallas import tpu as pltpu
from jax.sharding import PartitionSpec as P


CAP = 24

beta_one = 0.9
beta_two = 0.999
learn_rate = 0.01
decay_rate = 0.1
adam_eps = 1e-08
adam_count = 20.0

VMEM_LIMIT = 60 * 1024 * 1024


def adam_step(master, moment, second, gradient):
    moment_out = beta_one * moment + (1.0 - beta_one) * gradient
    second_out = beta_two * second + (1.0 - beta_two) * gradient * gradient
    scale_one = 1.0 - beta_one**adam_count
    scale_two = 1.0 - beta_two**adam_count
    update = moment_out / scale_one / (jnp.sqrt(second_out / scale_two) + adam_eps)
    master_out = master - learn_rate * (update + decay_rate * master)
    return (master_out, moment_out, second_out)


def keep_kernel(count, place_ref, routes_ref, probs_ref, tokens_ref, cot_ref, *out_refs):
    token_count = tokens_ref.shape[0]
    routes = routes_ref[...]
    probs = probs_ref[...]
    members = []
    factors = []
    for step in range(count):
        expert = lax.rem(place_ref[0] + step, count)
        picked = routes == expert
        members.append(jnp.sum(jnp.where(picked, 1.0, 0.0), axis=0, keepdims=True))
        factors.append(jnp.sum(jnp.where(picked, probs, 0.0), axis=0, keepdims=True))
    table = jnp.concatenate(members + [jnp.zeros_like(members[0])] * (-count % 8), axis=0)
    earlier = lax.broadcasted_iota(jnp.int32, (token_count, token_count), 0)
    later = lax.broadcasted_iota(jnp.int32, (token_count, token_count), 1)
    before = jnp.where(earlier < later, 1.0, 0.0).astype(jnp.bfloat16)
    ranked = jnp.dot(table.astype(jnp.bfloat16), before, preferred_element_type=jnp.float32)
    slots = lax.broadcasted_iota(jnp.int32, (CAP, token_count), 0).astype(jnp.float32)
    hits = []
    scales = []
    for step in range(count):
        hit = (members[step] > 0.5) & (ranked[step : step + 1] == slots)
        hits.append(jnp.where(hit, 1.0, 0.0))
        scales.append(jnp.sum(jnp.where(hit, factors[step], 0.0), axis=1, keepdims=True))
    one_hot = jnp.concatenate(hits, axis=0).astype(jnp.bfloat16)
    scale = jnp.concatenate(scales, axis=0)
    rows_in = jnp.dot(one_hot, tokens_ref[...], preferred_element_type=jnp.float32)
    rows_out = scale * jnp.dot(one_hot, cot_ref[...], preferred_element_type=jnp.float32)
    for step in range(count):
        span = slice(step * CAP, (step + 1) * CAP)
        out_refs[step][0] = rows_in[span].astype(jnp.bfloat16)
        out_refs[step][1] = rows_out[span].astype(jnp.bfloat16)


def keep_rows(tokens, cotangent, routes, probs, place, count):
    width = tokens.shape[1]
    vmem = pl.BlockSpec(memory_space=pltpu.VMEM)
    return pl.pallas_call(
        functools.partial(keep_kernel, count),
        out_shape=[jax.ShapeDtypeStruct((2, CAP, width), jnp.bfloat16)] * count,
        in_specs=[pl.BlockSpec(memory_space=pltpu.SMEM)] + [vmem] * 4,
        out_specs=[vmem] * count,
        cost_estimate=pl.CostEstimate(flops=4_000_000_000, bytes_accessed=2_000_000, transcendentals=0),
        name="keep_rows",
    )(place, routes.T, probs.T, tokens, cotangent)


def turn_kernel(parts, weight_ref, out_ref):
    half_width = weight_ref.shape[1] // 3
    units = half_width // parts
    if units % 16 == 0:
        turned = weight_ref[...].T
    else:
        turned = weight_ref[...].astype(jnp.float32).T
    for piece in range(parts):
        rows = [
            turned[kind * half_width + piece * units : kind * half_width + (piece + 1) * units]
            for kind in range(3)
        ]
        out_ref[piece] = jnp.concatenate(rows, axis=0).astype(jnp.bfloat16)


def turn_weights(weight, part, parts):
    width, columns = weight.shape
    span = width // 2
    block = min(256, span)
    steps = span // block
    return pl.pallas_call(
        functools.partial(turn_kernel, parts),
        out_shape=jax.ShapeDtypeStruct((parts, columns // parts, span), jnp.bfloat16),
        grid=(steps,),
        in_specs=[pl.BlockSpec((block, columns), lambda i: (part * steps + i, 0))],
        out_specs=pl.BlockSpec((parts, columns // parts, block), lambda i: (0, 0, i)),
        cost_estimate=pl.CostEstimate(flops=4_000_000_000, bytes_accessed=5_000_000, transcendentals=0),
        name="turn_weights",
    )(weight)


def grad_kernel(count, chunks, table_ref, own0_ref, own1_ref, far_ref, *refs):
    ins = refs[:count]
    outs = refs[count : 2 * count]
    grads = refs[2 * count : 2 * count + chunks]
    rows_in, rows_out, pair_w, down_w, pair_g, down_g, sems = refs[2 * count + chunks :]
    rows = ins[0].shape[0]
    units = down_w.shape[0] // 2
    span = own0_ref.shape[2]
    own_refs = (own0_ref, own1_ref)
    width = rows_in.shape[1]

    copies = []
    for index in range(count):
        place = pl.ds(index * rows, rows)
        copies.append(pltpu.make_async_copy(ins[index], rows_in.at[place], sems.at[0, index]))
        copies.append(pltpu.make_async_copy(outs[index], rows_out.at[place], sems.at[1, index]))
    for copy in copies:
        copy.start()

    for unit in range(4):
        half, part = unit // 2, unit % 2
        lanes = pl.ds(part * span, span)

        def fetch(source, unit=unit, half=half, lanes=lanes):
            one = pltpu.make_async_copy(
                source.at[pl.ds(0, 2 * units)],
                pair_w.at[pl.ds(2 * half * units, 2 * units), lanes],
                sems.at[2, 2 * unit],
            )
            two = pltpu.make_async_copy(
                source.at[pl.ds(2 * units, units)],
                down_w.at[pl.ds(half * units, units), lanes],
                sems.at[2, 2 * unit + 1],
            )
            one.start()
            two.start()
            one.wait()
            two.wait()

        @pl.when(table_ref[0, half] == 0)
        def _(half=half, part=part, fetch=fetch):
            fetch(own_refs[part].at[table_ref[1, half]])

        @pl.when(table_ref[0, half] != 0)
        def _(half=half, part=part, fetch=fetch):
            fetch(far_ref.at[half, part])

    for copy in copies:
        copy.wait()

    contract = (((1,), (1,)), ((), ()))
    pair = lax.dot_general(pair_w[...], rows_in[...], contract, preferred_element_type=jnp.float32)
    down = lax.dot_general(down_w[...], rows_out[...], contract, preferred_element_type=jnp.float32)
    for half in range(2):
        gate = pair[2 * half * units : (2 * half + 1) * units]
        up = pair[(2 * half + 1) * units : (2 * half + 2) * units]
        hidden_grad = down[half * units : (half + 1) * units]
        sig = jax.nn.sigmoid(gate)
        activated = gate * sig
        down_g[pl.ds(half * units, units)] = (activated * up).astype(jnp.bfloat16)
        gate_grad = hidden_grad * up * sig * (1.0 + gate * (1.0 - sig))
        pair_g[pl.ds(2 * half * units, 2 * units)] = jnp.concatenate(
            [gate_grad, hidden_grad * activated], axis=0
        ).astype(jnp.bfloat16)

    owners = grads[0].shape[0]
    block = width // owners
    lane = block // chunks

    def owner_step(owner, carry):
        place = pl.ds(pl.multiple_of(owner * block, block), block)
        grad_in = jnp.dot(pair_g[...], rows_in[:, place], preferred_element_type=jnp.float32)
        grad_out = jnp.dot(down_g[...], rows_out[:, place], preferred_element_type=jnp.float32)
        for chunk in range(chunks):
            part = slice(chunk * lane, (chunk + 1) * lane)
            for half in range(2):
                grads[chunk][owner, pl.ds(3 * half * units, 2 * units)] = grad_in[
                    2 * half * units : (2 * half + 2) * units, part
                ]
                grads[chunk][owner, pl.ds((3 * half + 2) * units, units)] = grad_out[
                    half * units : (half + 1) * units, part
                ]
        return carry

    lax.fori_loop(0, owners, owner_step, 0)


def half_grads(table, own, far, ins, outs, owners, chunks):
    count = len(ins)
    rows, width = ins[0].shape
    units = own[0].shape[1] // 3
    tokens = count * rows
    anywhere = pl.BlockSpec(memory_space=pl.ANY)
    lane = width // owners // chunks
    return pl.pallas_call(
        functools.partial(grad_kernel, count, chunks),
        out_shape=[jax.ShapeDtypeStruct((owners, 6 * units, lane), jnp.float32)] * chunks,
        in_specs=[pl.BlockSpec(memory_space=pltpu.SMEM)] + [anywhere] * (3 + 2 * count),
        out_specs=[pl.BlockSpec(memory_space=pltpu.VMEM)] * chunks,
        scratch_shapes=[
            pltpu.VMEM((tokens, width), jnp.bfloat16),
            pltpu.VMEM((tokens, width), jnp.bfloat16),
            pltpu.VMEM((4 * units, width), jnp.bfloat16),
            pltpu.VMEM((2 * units, width), jnp.bfloat16),
            pltpu.VMEM((4 * units, tokens), jnp.bfloat16),
            pltpu.VMEM((2 * units, tokens), jnp.bfloat16),
            pltpu.SemaphoreType.DMA((3, max(8, count))),
        ],
        compiler_params=pltpu.CompilerParams(vmem_limit_bytes=VMEM_LIMIT),
        cost_estimate=pl.CostEstimate(flops=10_000_000_000, bytes_accessed=10_000_000, transcendentals=0),
        name="half_grads",
    )(table, *own, far, *ins, *outs)


def update_kernel(sizes, held, arrived_ref, master_ref, moment_ref, second_ref, *out_refs):
    out_refs = out_refs[held:]
    parts, lines, _ = arrived_ref.shape
    units = lines // 6
    master_out, moment_out, second_out = out_refs[:3]
    fresh_refs = out_refs[3:]
    for half in range(2):
        stacked = jnp.concatenate(
            [
                arrived_ref[part, pl.ds((3 * half + kind) * units, units)]
                for kind in range(3)
                for part in range(parts)
            ],
            axis=0,
        )
        master, moment, second = adam_step(
            master_ref[half], moment_ref[half], second_ref[half], stacked.T
        )
        master_out[half] = master
        moment_out[half] = moment
        second_out[half] = second
        fresh = master.astype(jnp.bfloat16)
        begin = 0
        for index, size in enumerate(sizes):
            fresh_refs[2 * index + half][...] = fresh[begin : begin + size]
            begin += size


def update_rows(arrived, master, moment, second, chunk, sizes, held):
    lane = arrived.shape[2]
    columns = master.shape[2]
    state = pl.BlockSpec((2, lane, columns), lambda i: (0, chunk, 0))
    pieces = [size for size in sizes for _ in range(2)]
    return pl.pallas_call(
        functools.partial(update_kernel, sizes, len(held)),
        grid=(1,),
        out_shape=[jax.ShapeDtypeStruct(master.shape, jnp.float32)] * 3
        + [jax.ShapeDtypeStruct((size, columns), jnp.bfloat16) for size in pieces],
        in_specs=[pl.BlockSpec(arrived.shape, lambda i: (0, 0, 0)), state, state, state]
        + [pl.BlockSpec(memory_space=pl.ANY)] * len(held),
        out_specs=[state] * 3 + [pl.BlockSpec((size, columns), lambda i: (0, 0)) for size in pieces],
        input_output_aliases={4 + index: index for index in range(len(held))},
        compiler_params=pltpu.CompilerParams(vmem_limit_bytes=VMEM_LIMIT),
        cost_estimate=pl.CostEstimate(flops=4_000_000_000, bytes_accessed=9_000_000, transcendentals=0),
        name="update_rows",
    )(arrived, master, moment, second, *held)


def choose_kernel(count, want_ref, *refs):
    sources = refs[:count]
    out_ref = refs[count]
    for slot in range(out_ref.shape[0]):
        for index in range(count):

            @pl.when(want_ref[slot] == index)
            def _(slot=slot, index=index):
                out_ref[slot] = sources[index][...]


def choose_pieces(want, sources):
    count = len(sources)
    slots = want.shape[0]
    rows, columns = sources[0].shape
    vmem = pl.BlockSpec(memory_space=pltpu.VMEM)
    return pl.pallas_call(
        functools.partial(choose_kernel, count),
        out_shape=jax.ShapeDtypeStruct((slots, rows, columns), sources[0].dtype),
        in_specs=[pl.BlockSpec(memory_space=pltpu.SMEM)] + [vmem] * count,
        out_specs=vmem,
        compiler_params=pltpu.CompilerParams(vmem_limit_bytes=VMEM_LIMIT),
        cost_estimate=pl.CostEstimate(flops=1_500_000_000, bytes_accessed=4_000_000, transcendentals=0),
        name="choose_pieces",
    )(want, *sources)


def swap(value, mask, count):
    return lax.ppermute(value, "dp", [(i, i ^ mask) for i in range(count)])


def gather_rows(pieces, count):
    masks = [1 << bit for bit in range(count.bit_length() - 1)]
    while len(masks) >= 2:
        two, one = masks.pop(), masks.pop()
        grown = []
        for piece in pieces:
            first = [swap(half, one, count) for half in piece]
            other = [swap(half, two, count) for half in piece]
            far = (swap(first[0], two, count), swap(other[1], one, count))
            grown += [piece, tuple(first), tuple(other), far]
        pieces = grown
    if masks:
        pieces = pieces + [tuple(swap(half, masks[0], count) for half in piece) for piece in pieces]
    return pieces


def step_body(tokens, cotangent, routes, probs, replicas, hold_now, hold_next, master, moment, second):
    planes = lax.axis_size("expert")
    columns = lax.axis_size("dp")
    devices = planes * columns
    width = tokens.shape[1]
    block_rows = width // columns
    plane = lax.axis_index("expert")

    kept = keep_rows(tokens, cotangent, routes, probs, plane.reshape(1), planes)
    came = [kept[0]] + [
        lax.ppermute(kept[step], "expert", [(i, (i + step) % planes) for i in range(planes)])
        for step in range(1, planes)
    ]

    flat = hold_now.reshape(devices)
    ids = jnp.arange(devices, dtype=jnp.int32)
    pieces_ids = jnp.arange(2 * planes, dtype=jnp.int32)
    apart = jnp.abs(ids[None, :] // columns - pieces_ids[:, None] // 2)
    order = jnp.where(flat[None, :] == pieces_ids[:, None], apart * devices + ids[None, :], devices * devices)
    holder = jnp.min(order, axis=1) % devices
    from_plane = (holder // columns).reshape(planes, 2)
    from_column = (holder % columns).reshape(planes, 2)
    shift = jnp.arange(planes, dtype=jnp.int32)[:, None] - from_plane

    own = []
    for part in range(2):
        turned = turn_weights(replicas[0, 0], part, columns)
        own.append(lax.all_to_all(turned, "dp", split_axis=0, concat_axis=0, tiled=True))
    own = tuple(own)

    first = (
        jnp.concatenate([rows[0] for rows in came], axis=0),
        jnp.concatenate([rows[1] for rows in came], axis=0),
    )
    state = tuple(jnp.transpose(part[0], (1, 0, 2)) for part in (master, moment, second))
    (first, own, state) = lax.optimization_barrier((first, own, state))
    signs = jnp.array([1, -1], jnp.int32)[:, None, None]
    steps = jnp.arange(1, planes, dtype=jnp.int32)[None, :, None]
    experts = jnp.arange(planes, dtype=jnp.int32)
    needs = shift[None, None] == (signs * steps)[..., None]
    trips = jnp.max(jnp.sum(needs.astype(jnp.int32), axis=3), axis=(0, 2))
    reached = (experts[None, None, :] == plane + signs * steps)[..., None]
    need_there = jnp.any(needs & reached, axis=2)
    column_there = jnp.sum(jnp.where(reached, from_column[None, None], 0), axis=2)
    send_column = jnp.stack(
        [jnp.where(need_there[..., 0], column_there[..., 0], column_there[..., 1]), column_there[..., 1]],
        axis=2,
    )
    here = (experts == plane)[:, None]
    need_here = jnp.any(needs & here[None, None], axis=2)
    first_here, last_here = need_here[..., 0], need_here[..., 1]
    none_here = jnp.zeros_like(first_here)
    takes = jnp.stack(
        [
            jnp.stack([first_here, last_here & ~first_here], axis=2),
            jnp.stack([none_here, last_here & first_here], axis=2),
        ],
        axis=2,
    )
    side = jnp.any(jnp.where(here, shift, 0) != 0, axis=0).astype(jnp.int32)
    table = jnp.stack([side, jnp.sum(jnp.where(here, from_column, 0), axis=0)])

    far = jnp.zeros((2, 2) + own[0].shape[1:], own[0].dtype)
    for step in range(1, planes):

        def trip(index, kept_far, step=step):
            for sign_index, sign in enumerate((1, -1)):
                source = send_column[sign_index, step - 1, index]
                pairs = [(i, i + sign * step) for i in range(planes) if 0 <= i + sign * step < planes]
                sent = jnp.stack(
                    [lax.dynamic_index_in_dim(part, source, 0, keepdims=False) for part in own]
                )
                got = lax.ppermute(sent, "expert", pairs)
                take = takes[sign_index, step - 1, index]
                kept_far = jnp.where(take[:, None, None, None], got[None], kept_far)
            return kept_far

        far = lax.fori_loop(0, trips[step - 1], trip, far)

    rows = gather_rows([first], columns)

    chunks = max(1, block_rows // 128)
    partial = half_grads(
        table, own, far, [r[0] for r in rows], [r[1] for r in rows], columns, chunks
    )
    lane = block_rows // chunks
    updated = []
    fresh = []
    for chunk in range(chunks):
        arrived = lax.all_to_all(partial[chunk], "dp", split_axis=0, concat_axis=0, tiled=True)
        cut = lane * 5 // 8 // 16 * 16
        sizes = [lane] if chunk + 1 < chunks or cut == 0 else [cut, lane - cut]
        result = update_rows(arrived, *state, chunk, sizes, updated)
        updated = result[:3]
        fresh += [(result[3 + 2 * i], result[4 + 2 * i]) for i in range(len(sizes))]

    next_row = lax.dynamic_index_in_dim(hold_next, plane, 0, keepdims=False)
    next_plane = next_row // 2
    next_half = next_row % 2
    turns = jnp.where(next_half == 0, plane - next_plane, next_plane - plane)
    want = (next_half * planes + (turns + planes) % planes).astype(jnp.int32)
    forward = [(i, (i + 1) % planes) for i in range(planes)]
    backward = [(i, (i - 1) % planes) for i in range(planes)]
    outs = []
    for kind in range(3):
        out = jnp.transpose(updated[kind], (1, 0, 2))[None]
        outs.append(out)
    replica = None
    begin = 0
    for own_halves in fresh:
        rings = [[own_halves[0]], [own_halves[1]]]
        for _ in range(1, planes):
            rings[0].append(lax.ppermute(rings[0][-1], "expert", forward))
            rings[1].append(lax.ppermute(rings[1][-1], "expert", backward))
        sources = rings[0] + rings[1]
        outgoing = choose_pieces(want, sources)
        arrived = lax.all_to_all(outgoing, "dp", split_axis=0, concat_axis=0, tiled=True)
        if replica is None:
            replica = jnp.zeros((columns, block_rows, arrived.shape[2]), arrived.dtype)
        replica = lax.dynamic_update_slice(replica, arrived, (0, begin, 0))
        begin += own_halves[0].shape[0]
    next_replicas = replica.reshape(1, 1, width, replica.shape[2])

    return (*outs, next_replicas)


def solution(mesh):
    placed = (
        P(("expert", "dp"), None),
        P(("expert", "dp"), None),
        P(("expert", "dp"), None),
        P(("expert", "dp"), None),
        P("expert", "dp", None, None),
        P(),
        P(),
        P("expert", "dp", None, None),
        P("expert", "dp", None, None),
        P("expert", "dp", None, None),
    )
    return jax.shard_map(
        step_body,
        mesh=mesh,
        in_specs=placed,
        out_specs=(P("expert", "dp", None, None),) * 4,
        check_vma=False,
    )
```

```python
import functools

import jax
import jax.numpy as jnp
from jax import lax
from jax.experimental import pallas as pl
from jax.experimental.pallas import tpu as pltpu
from jax.sharding import PartitionSpec as P


CAP = 24

beta_one = 0.9
beta_two = 0.999
learn_rate = 0.01
decay_rate = 0.1
adam_eps = 1e-08
adam_count = 20.0

VMEM_LIMIT = 60 * 1024 * 1024


def adam_step(master, moment, second, gradient):
    moment_out = beta_one * moment + (1.0 - beta_one) * gradient
    second_out = beta_two * second + (1.0 - beta_two) * gradient * gradient
    scale_one = 1.0 - beta_one**adam_count
    scale_two = 1.0 - beta_two**adam_count
    update = moment_out / scale_one / (jnp.sqrt(second_out / scale_two) + adam_eps)
    master_out = master - learn_rate * (update + decay_rate * master)
    return (master_out, moment_out, second_out)


def keep_kernel(count, place_ref, routes_ref, probs_ref, tokens_ref, cot_ref, *out_refs):
    token_count = tokens_ref.shape[0]
    routes = routes_ref[...]
    probs = probs_ref[...]
    members = []
    factors = []
    for step in range(count):
        expert = lax.rem(place_ref[0] + step, count)
        picked = routes == expert
        members.append(jnp.sum(jnp.where(picked, 1.0, 0.0), axis=0, keepdims=True))
        factors.append(jnp.sum(jnp.where(picked, probs, 0.0), axis=0, keepdims=True))
    table = jnp.concatenate(members + [jnp.zeros_like(members[0])] * (-count % 8), axis=0)
    earlier = lax.broadcasted_iota(jnp.int32, (token_count, token_count), 0)
    later = lax.broadcasted_iota(jnp.int32, (token_count, token_count), 1)
    before = jnp.where(earlier < later, 1.0, 0.0).astype(jnp.bfloat16)
    ranked = jnp.dot(table.astype(jnp.bfloat16), before, preferred_element_type=jnp.float32)
    slots = lax.broadcasted_iota(jnp.int32, (CAP, token_count), 0).astype(jnp.float32)
    hits = []
    scales = []
    for step in range(count):
        hit = (members[step] > 0.5) & (ranked[step : step + 1] == slots)
        hits.append(jnp.where(hit, 1.0, 0.0))
        scales.append(jnp.sum(jnp.where(hit, factors[step], 0.0), axis=1, keepdims=True))
    one_hot = jnp.concatenate(hits, axis=0).astype(jnp.bfloat16)
    scale = jnp.concatenate(scales, axis=0)
    rows_in = jnp.dot(one_hot, tokens_ref[...], preferred_element_type=jnp.float32)
    rows_out = scale * jnp.dot(one_hot, cot_ref[...], preferred_element_type=jnp.float32)
    for step in range(count):
        span = slice(step * CAP, (step + 1) * CAP)
        out_refs[step][0] = rows_in[span].astype(jnp.bfloat16)
        out_refs[step][1] = rows_out[span].astype(jnp.bfloat16)


def keep_rows(tokens, cotangent, routes, probs, place, count):
    width = tokens.shape[1]
    vmem = pl.BlockSpec(memory_space=pltpu.VMEM)
    return pl.pallas_call(
        functools.partial(keep_kernel, count),
        out_shape=[jax.ShapeDtypeStruct((2, CAP, width), jnp.bfloat16)] * count,
        in_specs=[pl.BlockSpec(memory_space=pltpu.SMEM)] + [vmem] * 4,
        out_specs=[vmem] * count,
        cost_estimate=pl.CostEstimate(flops=4_000_000_000, bytes_accessed=2_000_000, transcendentals=0),
        name="keep_rows",
    )(place, routes.T, probs.T, tokens, cotangent)


def turn_kernel(parts, weight_ref, out_ref):
    half_width = weight_ref.shape[1] // 3
    units = half_width // parts
    if units % 16 == 0:
        turned = weight_ref[...].T
    else:
        turned = weight_ref[...].astype(jnp.float32).T
    for piece in range(parts):
        rows = [
            turned[kind * half_width + piece * units : kind * half_width + (piece + 1) * units]
            for kind in range(3)
        ]
        out_ref[piece] = jnp.concatenate(rows, axis=0).astype(jnp.bfloat16)


def turn_weights(weight, part, parts):
    width, columns = weight.shape
    span = width // 2
    block = min(256, span)
    steps = span // block
    return pl.pallas_call(
        functools.partial(turn_kernel, parts),
        out_shape=jax.ShapeDtypeStruct((parts, columns // parts, span), jnp.bfloat16),
        grid=(steps,),
        in_specs=[pl.BlockSpec((block, columns), lambda i: (part * steps + i, 0))],
        out_specs=pl.BlockSpec((parts, columns // parts, block), lambda i: (0, 0, i)),
        cost_estimate=pl.CostEstimate(flops=4_000_000_000, bytes_accessed=5_000_000, transcendentals=0),
        name="turn_weights",
    )(weight)


def grad_kernel(count, chunks, table_ref, own0_ref, own1_ref, far_ref, *refs):
    ins = refs[:count]
    outs = refs[count : 2 * count]
    grads = refs[2 * count : 2 * count + chunks]
    rows_in, rows_out, pair_w, down_w, pair_g, down_g, sems = refs[2 * count + chunks :]
    rows = ins[0].shape[0]
    units = down_w.shape[0] // 2
    span = own0_ref.shape[2]
    own_refs = (own0_ref, own1_ref)
    width = rows_in.shape[1]

    copies = []
    for index in range(count):
        place = pl.ds(index * rows, rows)
        copies.append(pltpu.make_async_copy(ins[index], rows_in.at[place], sems.at[0, index]))
        copies.append(pltpu.make_async_copy(outs[index], rows_out.at[place], sems.at[1, index]))
    for copy in copies:
        copy.start()

    for unit in range(4):
        half, part = unit // 2, unit % 2
        lanes = pl.ds(part * span, span)

        def fetch(source, unit=unit, half=half, lanes=lanes):
            one = pltpu.make_async_copy(
                source.at[pl.ds(0, 2 * units)],
                pair_w.at[pl.ds(2 * half * units, 2 * units), lanes],
                sems.at[2, 2 * unit],
            )
            two = pltpu.make_async_copy(
                source.at[pl.ds(2 * units, units)],
                down_w.at[pl.ds(half * units, units), lanes],
                sems.at[2, 2 * unit + 1],
            )
            one.start()
            two.start()
            one.wait()
            two.wait()

        @pl.when(table_ref[0, half] == 0)
        def _(half=half, part=part, fetch=fetch):
            fetch(own_refs[part].at[table_ref[1, half]])

        @pl.when(table_ref[0, half] != 0)
        def _(half=half, part=part, fetch=fetch):
            fetch(far_ref.at[half, part])

    for copy in copies:
        copy.wait()

    contract = (((1,), (1,)), ((), ()))
    pair = lax.dot_general(pair_w[...], rows_in[...], contract, preferred_element_type=jnp.float32)
    down = lax.dot_general(down_w[...], rows_out[...], contract, preferred_element_type=jnp.float32)
    for half in range(2):
        gate = pair[2 * half * units : (2 * half + 1) * units]
        up = pair[(2 * half + 1) * units : (2 * half + 2) * units]
        hidden_grad = down[half * units : (half + 1) * units]
        sig = jax.nn.sigmoid(gate)
        activated = gate * sig
        down_g[pl.ds(half * units, units)] = (activated * up).astype(jnp.bfloat16)
        gate_grad = hidden_grad * up * sig * (1.0 + gate * (1.0 - sig))
        pair_g[pl.ds(2 * half * units, 2 * units)] = jnp.concatenate(
            [gate_grad, hidden_grad * activated], axis=0
        ).astype(jnp.bfloat16)

    owners = grads[0].shape[0]
    block = width // owners
    lane = block // chunks

    def owner_step(owner, carry):
        place = pl.ds(pl.multiple_of(owner * block, block), block)
        grad_in = jnp.dot(pair_g[...], rows_in[:, place], preferred_element_type=jnp.float32)
        grad_out = jnp.dot(down_g[...], rows_out[:, place], preferred_element_type=jnp.float32)
        for chunk in range(chunks):
            part = slice(chunk * lane, (chunk + 1) * lane)
            for half in range(2):
                grads[chunk][owner, pl.ds(3 * half * units, 2 * units)] = grad_in[
                    2 * half * units : (2 * half + 2) * units, part
                ]
                grads[chunk][owner, pl.ds((3 * half + 2) * units, units)] = grad_out[
                    half * units : (half + 1) * units, part
                ]
        return carry

    lax.fori_loop(0, owners, owner_step, 0)


def half_grads(table, own, far, ins, outs, owners, chunks):
    count = len(ins)
    rows, width = ins[0].shape
    units = own[0].shape[1] // 3
    tokens = count * rows
    anywhere = pl.BlockSpec(memory_space=pl.ANY)
    lane = width // owners // chunks
    return pl.pallas_call(
        functools.partial(grad_kernel, count, chunks),
        out_shape=[jax.ShapeDtypeStruct((owners, 6 * units, lane), jnp.float32)] * chunks,
        in_specs=[pl.BlockSpec(memory_space=pltpu.SMEM)] + [anywhere] * (3 + 2 * count),
        out_specs=[pl.BlockSpec(memory_space=pltpu.VMEM)] * chunks,
        scratch_shapes=[
            pltpu.VMEM((tokens, width), jnp.bfloat16),
            pltpu.VMEM((tokens, width), jnp.bfloat16),
            pltpu.VMEM((4 * units, width), jnp.bfloat16),
            pltpu.VMEM((2 * units, width), jnp.bfloat16),
            pltpu.VMEM((4 * units, tokens), jnp.bfloat16),
            pltpu.VMEM((2 * units, tokens), jnp.bfloat16),
            pltpu.SemaphoreType.DMA((3, max(8, count))),
        ],
        compiler_params=pltpu.CompilerParams(vmem_limit_bytes=VMEM_LIMIT),
        cost_estimate=pl.CostEstimate(flops=10_000_000_000, bytes_accessed=10_000_000, transcendentals=0),
        name="half_grads",
    )(table, *own, far, *ins, *outs)


def update_kernel(sizes, held, arrived_ref, master_ref, moment_ref, second_ref, *out_refs):
    out_refs = out_refs[held:]
    parts, lines, _ = arrived_ref.shape
    units = lines // 6
    master_out, moment_out, second_out = out_refs[:3]
    fresh_refs = out_refs[3:]
    for half in range(2):
        stacked = jnp.concatenate(
            [
                arrived_ref[part, pl.ds((3 * half + kind) * units, units)]
                for kind in range(3)
                for part in range(parts)
            ],
            axis=0,
        )
        master, moment, second = adam_step(
            master_ref[half], moment_ref[half], second_ref[half], stacked.T
        )
        master_out[half] = master
        moment_out[half] = moment
        second_out[half] = second
        fresh = master.astype(jnp.bfloat16)
        begin = 0
        for index, size in enumerate(sizes):
            fresh_refs[2 * index + half][...] = fresh[begin : begin + size]
            begin += size


def update_rows(arrived, master, moment, second, chunk, sizes, held):
    lane = arrived.shape[2]
    columns = master.shape[2]
    state = pl.BlockSpec((2, lane, columns), lambda i: (0, chunk, 0))
    pieces = [size for size in sizes for _ in range(2)]
    return pl.pallas_call(
        functools.partial(update_kernel, sizes, len(held)),
        grid=(1,),
        out_shape=[jax.ShapeDtypeStruct(master.shape, jnp.float32)] * 3
        + [jax.ShapeDtypeStruct((size, columns), jnp.bfloat16) for size in pieces],
        in_specs=[pl.BlockSpec(arrived.shape, lambda i: (0, 0, 0)), state, state, state]
        + [pl.BlockSpec(memory_space=pl.ANY)] * len(held),
        out_specs=[state] * 3 + [pl.BlockSpec((size, columns), lambda i: (0, 0)) for size in pieces],
        input_output_aliases={4 + index: index for index in range(len(held))},
        compiler_params=pltpu.CompilerParams(vmem_limit_bytes=VMEM_LIMIT),
        cost_estimate=pl.CostEstimate(flops=4_000_000_000, bytes_accessed=9_000_000, transcendentals=0),
        name="update_rows",
    )(arrived, master, moment, second, *held)


def join_kernel(halves_ref, out_ref):
    for half in range(2):
        out_ref[:, half, :] = halves_ref[half]


def join_halves(halves):
    _, rows, columns = halves.shape
    block = min(64, rows)
    return pl.pallas_call(
        join_kernel,
        grid=(rows // block,),
        out_shape=jax.ShapeDtypeStruct((rows, 2, columns), halves.dtype),
        in_specs=[pl.BlockSpec((2, block, columns), lambda i: (0, i, 0))],
        out_specs=pl.BlockSpec((block, 2, columns), lambda i: (i, 0, 0)),
        cost_estimate=pl.CostEstimate(flops=2_000_000_000, bytes_accessed=5_000_000, transcendentals=0),
        name="join_halves",
    )(halves)


def choose_kernel(count, want_ref, *refs):
    sources = refs[:count]
    out_ref = refs[count]
    for slot in range(out_ref.shape[0]):
        for index in range(count):

            @pl.when(want_ref[slot] == index)
            def _(slot=slot, index=index):
                out_ref[slot] = sources[index][...]


def choose_pieces(want, sources):
    count = len(sources)
    slots = want.shape[0]
    rows, columns = sources[0].shape
    vmem = pl.BlockSpec(memory_space=pltpu.VMEM)
    return pl.pallas_call(
        functools.partial(choose_kernel, count),
        out_shape=jax.ShapeDtypeStruct((slots, rows, columns), sources[0].dtype),
        in_specs=[pl.BlockSpec(memory_space=pltpu.SMEM)] + [vmem] * count,
        out_specs=vmem,
        compiler_params=pltpu.CompilerParams(vmem_limit_bytes=VMEM_LIMIT),
        cost_estimate=pl.CostEstimate(flops=1_500_000_000, bytes_accessed=4_000_000, transcendentals=0),
        name="choose_pieces",
    )(want, *sources)


def swap(value, mask, count):
    return lax.ppermute(value, "dp", [(i, i ^ mask) for i in range(count)])


def gather_rows(pieces, count):
    masks = [1 << bit for bit in range(count.bit_length() - 1)]
    while len(masks) >= 2:
        two, one = masks.pop(), masks.pop()
        grown = []
        for piece in pieces:
            first = [swap(half, one, count) for half in piece]
            other = [swap(half, two, count) for half in piece]
            far = (swap(first[0], two, count), swap(other[1], one, count))
            grown += [piece, tuple(first), tuple(other), far]
        pieces = grown
    if masks:
        pieces = pieces + [tuple(swap(half, masks[0], count) for half in piece) for piece in pieces]
    return pieces


def step_body(tokens, cotangent, routes, probs, replicas, hold_now, hold_next, master, moment, second):
    planes = lax.axis_size("expert")
    columns = lax.axis_size("dp")
    devices = planes * columns
    width = tokens.shape[1]
    block_rows = width // columns
    plane = lax.axis_index("expert")

    kept = keep_rows(tokens, cotangent, routes, probs, plane.reshape(1), planes)
    came = [kept[0]] + [
        lax.ppermute(kept[step], "expert", [(i, (i + step) % planes) for i in range(planes)])
        for step in range(1, planes)
    ]

    flat = hold_now.reshape(devices)
    ids = jnp.arange(devices, dtype=jnp.int32)
    pieces_ids = jnp.arange(2 * planes, dtype=jnp.int32)
    apart = jnp.abs(ids[None, :] // columns - pieces_ids[:, None] // 2)
    order = jnp.where(flat[None, :] == pieces_ids[:, None], apart * devices + ids[None, :], devices * devices)
    holder = jnp.min(order, axis=1) % devices
    from_plane = (holder // columns).reshape(planes, 2)
    from_column = (holder % columns).reshape(planes, 2)
    shift = jnp.arange(planes, dtype=jnp.int32)[:, None] - from_plane

    own = []
    for part in range(2):
        turned = turn_weights(replicas[0, 0], part, columns)
        own.append(lax.all_to_all(turned, "dp", split_axis=0, concat_axis=0, tiled=True))
    own = tuple(own)

    first = (
        jnp.concatenate([rows[0] for rows in came], axis=0),
        jnp.concatenate([rows[1] for rows in came], axis=0),
    )
    state = tuple(jnp.transpose(part[0], (1, 0, 2)) for part in (master, moment, second))
    (first, own, state) = lax.optimization_barrier((first, own, state))
    signs = jnp.array([1, -1], jnp.int32)[:, None, None]
    steps = jnp.arange(1, planes, dtype=jnp.int32)[None, :, None]
    experts = jnp.arange(planes, dtype=jnp.int32)
    needs = shift[None, None] == (signs * steps)[..., None]
    trips = jnp.max(jnp.sum(needs.astype(jnp.int32), axis=3), axis=(0, 2))
    reached = (experts[None, None, :] == plane + signs * steps)[..., None]
    need_there = jnp.any(needs & reached, axis=2)
    column_there = jnp.sum(jnp.where(reached, from_column[None, None], 0), axis=2)
    send_column = jnp.stack(
        [jnp.where(need_there[..., 0], column_there[..., 0], column_there[..., 1]), column_there[..., 1]],
        axis=2,
    )
    here = (experts == plane)[:, None]
    need_here = jnp.any(needs & here[None, None], axis=2)
    first_here, last_here = need_here[..., 0], need_here[..., 1]
    none_here = jnp.zeros_like(first_here)
    takes = jnp.stack(
        [
            jnp.stack([first_here, last_here & ~first_here], axis=2),
            jnp.stack([none_here, last_here & first_here], axis=2),
        ],
        axis=2,
    )
    side = jnp.any(jnp.where(here, shift, 0) != 0, axis=0).astype(jnp.int32)
    table = jnp.stack([side, jnp.sum(jnp.where(here, from_column, 0), axis=0)])

    far = jnp.zeros((2, 2) + own[0].shape[1:], own[0].dtype)
    for step in range(1, planes):

        def trip(index, kept_far, step=step):
            for sign_index, sign in enumerate((1, -1)):
                source = send_column[sign_index, step - 1, index]
                pairs = [(i, i + sign * step) for i in range(planes) if 0 <= i + sign * step < planes]
                sent = jnp.stack(
                    [lax.dynamic_index_in_dim(part, source, 0, keepdims=False) for part in own]
                )
                got = lax.ppermute(sent, "expert", pairs)
                take = takes[sign_index, step - 1, index]
                kept_far = jnp.where(take[:, None, None, None], got[None], kept_far)
            return kept_far

        far = lax.fori_loop(0, trips[step - 1], trip, far)

    rows = gather_rows([first], columns)

    chunks = max(1, block_rows // 128)
    partial = half_grads(
        table, own, far, [r[0] for r in rows], [r[1] for r in rows], columns, chunks
    )
    lane = block_rows // chunks
    updated = []
    fresh = []
    for chunk in range(chunks):
        arrived = lax.all_to_all(partial[chunk], "dp", split_axis=0, concat_axis=0, tiled=True)
        cut = lane * 5 // 8 // 16 * 16
        sizes = [lane] if chunk + 1 < chunks or cut == 0 else [cut, lane - cut]
        result = update_rows(arrived, *state, chunk, sizes, updated)
        updated = result[:3]
        fresh += [(result[3 + 2 * i], result[4 + 2 * i]) for i in range(len(sizes))]

    next_row = lax.dynamic_index_in_dim(hold_next, plane, 0, keepdims=False)
    next_plane = next_row // 2
    next_half = next_row % 2
    turns = jnp.where(next_half == 0, plane - next_plane, next_plane - plane)
    want = (next_half * planes + (turns + planes) % planes).astype(jnp.int32)
    forward = [(i, (i + 1) % planes) for i in range(planes)]
    backward = [(i, (i - 1) % planes) for i in range(planes)]
    outs = []
    for kind in range(3):
        outs.append(join_halves(updated[kind])[None])
    replica = None
    begin = 0
    for own_halves in fresh:
        rings = [[own_halves[0]], [own_halves[1]]]
        for _ in range(1, planes):
            rings[0].append(lax.ppermute(rings[0][-1], "expert", forward))
            rings[1].append(lax.ppermute(rings[1][-1], "expert", backward))
        sources = rings[0] + rings[1]
        outgoing = choose_pieces(want, sources)
        arrived = lax.all_to_all(outgoing, "dp", split_axis=0, concat_axis=0, tiled=True)
        if replica is None:
            replica = jnp.zeros((columns, block_rows, arrived.shape[2]), arrived.dtype)
        replica = lax.dynamic_update_slice(replica, arrived, (0, begin, 0))
        begin += own_halves[0].shape[0]
    next_replicas = replica.reshape(1, 1, width, replica.shape[2])

    return (*outs, next_replicas)


def solution(mesh):
    placed = (
        P(("expert", "dp"), None),
        P(("expert", "dp"), None),
        P(("expert", "dp"), None),
        P(("expert", "dp"), None),
        P("expert", "dp", None, None),
        P(),
        P(),
        P("expert", "dp", None, None),
        P("expert", "dp", None, None),
        P("expert", "dp", None, None),
    )
    return jax.shard_map(
        step_body,
        mesh=mesh,
        in_specs=placed,
        out_specs=(P("expert", "dp", None, None),) * 4,
        check_vma=False,
    )
```
